32 devices in a mesh: ep: 8 (over z, x), fsdp: 4 (over y, core).
Axes of the slice: x: 2, y: 2, z: 4, core: 2. Of those that a mesh axis runs over, the one named last changes fastest.
Arguments:
- train_down: float32 [64, 1408, 2048], P('ep', None, 'fsdp'), may hold values from -0.21875 to 0.21875
- other_down: float32 [64, 1408, 2048], P('ep', None, 'fsdp'), may hold values from -0.15625 to 0.15625
- router_weight: float32 [2048, 64], P('fsdp', 'ep'), may hold values from -0.125 to 0.125
- router_gain: float32 [2048], P('fsdp'), may hold values from 0.25 to 1.75
Outputs:
- ready_down: bfloat16 [64, 1408, 2048], P('ep')
- scale_down: float32 [64, 1408], P('ep')
- serve_router: bfloat16 [2048, 64], replicated
- latest_down: float32 [64, 1408, 2048], P('ep', None, 'fsdp')
The draws below stay inside these ranges and needn't reach their ends.
All inputs are finite; a program needn't handle non-finite values.
Results may differ from the reference program's by a relative error of at most 0.001.
Values may be sent and summed in bfloat16 or wider, within the bound.
No kernel may reach another device: no remote copies, remote signals or barrier semaphores. Data moves between devices by JAX's collectives and lax.ppermute only.
A program may use at most 256 MiB of HBM per device.

```python
import jax
import jax.numpy as jnp
from jax import lax

EXPERTS = 64
D_MODEL = 2048
D_EXPERT = 1408


def raised(values, stream_key, source, target, shards_of, factor):
    def block_of(axis_at):
        return (jnp.arange(values.shape[axis_at]) // (values.shape[axis_at] // shards_of)).reshape((-1,) + (1,) * (values.ndim - 1 - axis_at))

    first = jax.random.permutation(stream_key, shards_of)[block_of(target)]
    other_side = (block_of(target) + shards_of // 2) % shards_of
    return jnp.where((block_of(source) == first) | (block_of(source) == other_side), factor * values, values)


def levels(own_key, dims, pieces, smallest, top_value):
    level = 1.0
    for dim, shards_of in pieces:
        heights = jax.random.uniform(jax.random.fold_in(jax.random.fold_in(own_key, 6), dim), (shards_of,), jnp.float32, smallest / len(pieces), top_value / len(pieces))
        level = level * jnp.repeat(jnp.exp(heights), dims[dim] // shards_of).reshape((-1,) + (1,) * (len(dims) - 1 - dim))
    return level


def scatter_about(rng, dims, spread, bound, cuts=(), held_as=jnp.bfloat16):
    gain = levels(rng, dims, cuts, -0.22, 0.18) if cuts else 1.0
    array = jax.random.normal(rng, dims, jnp.float32) * spread * gain
    return jnp.minimum(jnp.maximum(array, -bound), bound).astype(held_as)


def heavy_noise(key, extent, spread, limit, pieces, heavy, kind=jnp.bfloat16):
    drawn = spread * jax.random.normal(key, extent, jnp.float32)
    if pieces:
        drawn = drawn * levels(key, extent, pieces, -0.22, 0.18)
    return jnp.clip(raised(drawn, jax.random.fold_in(key, 3), *heavy), -limit, limit).astype(kind)


def setup_inputs(seed: int = 0) -> dict:
    arg_keys = jax.random.split(jax.random.key(seed), 5)
    return {
        "train_down": heavy_noise(arg_keys[0], (EXPERTS, D_EXPERT, D_MODEL), D_EXPERT ** -0.5, 0.21875, ((0, 8), (2, 4)), (2, 1, 4, 2.0), jnp.float32),
        "other_down": scatter_about(arg_keys[1], (EXPERTS, D_EXPERT, D_MODEL), D_EXPERT ** -0.5, 0.15625, ((0, 8), (2, 4)), jnp.float32),
        "router_weight": scatter_about(arg_keys[2], (D_MODEL, EXPERTS), D_MODEL ** -0.5, 0.125, ((0, 4), (1, 8)), jnp.float32),
        "router_gain": jnp.clip(1.0 + 0.15 * jax.random.normal(arg_keys[3], (D_MODEL,), jnp.float32), 0.25, 1.75),
    }


def reference(train_down, other_down, router_weight, router_gain):
    latest_down = 0.5 * other_down + 0.5 * train_down
    scale_down = jnp.sqrt(lax.optimization_barrier(jnp.sum(latest_down * latest_down, axis=2)))
    ready_down = (latest_down / jnp.expand_dims(scale_down, 2)).astype(jnp.bfloat16)
    serve_router = (router_weight * router_gain[:, None]).astype(jnp.bfloat16)
    return (ready_down, scale_down, serve_router, latest_down)
```

```python
import functools

import jax
import jax.numpy as jnp
from jax import lax
from jax.experimental import pallas as pl
from jax.experimental.pallas import tpu as pltpu
from jax.sharding import PartitionSpec as P


PARTS = 16
PIECES = (1, 1, 2, 2, 2, 2, 2, 2, 1, 1)
FIRST = 3


def place_kernel(count, columns_ref, *refs):
    ready_ref = refs[-1]
    for index in range(count):
        width = refs[index].shape[1]
        start = pl.multiple_of(columns_ref[index] * width, width)
        ready_ref[:, pl.ds(start, width)] = refs[index][...]


def place(columns, blocks, ready, start, rows, step):
    count = len(blocks)
    size, width = blocks[0].shape
    at = start // step
    in_specs = [pl.BlockSpec((step, width), lambda i, c: (i, 0)) for _ in blocks]
    args = [columns, *blocks]
    aliases = {}
    if ready is not None:
        in_specs.append(pl.BlockSpec(memory_space=pl.ANY))
        args.append(ready)
        aliases = {count + 1: 0}
    return pl.pallas_call(
        functools.partial(place_kernel, count),
        grid_spec=pltpu.PrefetchScalarGridSpec(
            num_scalar_prefetch=1,
            grid=(size // step,),
            in_specs=in_specs,
            out_specs=pl.BlockSpec((step, count * width), lambda i, c: (at + i, 0)),
        ),
        out_shape=jax.ShapeDtypeStruct((rows, count * width), blocks[0].dtype),
        input_output_aliases=aliases,
        cost_estimate=pl.CostEstimate(
            flops=4 * size * count * width,
            bytes_accessed=4 * size * count * width,
            transcendentals=0,
        ),
    )(*args)


def on_device(n, train_down, other_down, router_weight, router_gain):
    experts, inner, width = train_down.shape
    rows = experts * inner
    chips = n // 2
    me = lax.axis_index("fsdp")

    def send(values, hop, swap):
        pairs = [(i, ((i // 2 + hop) % chips) * 2 + ((i % 2) ^ swap)) for i in range(n)]
        return lax.ppermute(values, "fsdp", pairs)

    hops = [(hop, swap) for hop in range(chips) for swap in range(2)]
    behind = jnp.array([chips - hop for hop, _ in hops], jnp.int32) + (me >> 1)
    behind = jnp.where(behind >= chips, behind - chips, behind)
    columns = behind * 2 + ((me & 1) ^ jnp.array([swap for _, swap in hops], jnp.int32))

    def total(part):
        if n != 4:
            return lax.psum(part, "fsdp")
        near = part + send(part, 0, 1)
        far = send(part, 1, 0) + send(part, 1, 1)
        return near + far

    train = train_down.reshape(rows, width)
    other = other_down.reshape(rows, width)

    def latest(first, last, train, other):
        return 0.5 * other[first:last] + 0.5 * train[first:last]

    def squares(first, last, train, other):
        part = latest(first, last, train, other)
        return jnp.sum(part * part, axis=1)

    unit = rows // PARTS
    step = unit // 2 if unit % 32 == 0 else unit
    edges = [0]
    for piece in PIECES:
        edges.append(edges[-1] + piece * unit)
    split = edges[FIRST]

    def narrow(index, scale, base, train, other):
        first, last = edges[index], edges[index + 1]
        return (latest(first, last, train, other) / scale[first - base:last - base, None]).astype(jnp.bfloat16)

    part_router = (router_weight * router_gain[:, None]).astype(jnp.bfloat16).T
    router_blocks = [part_router if hop == (0, 0) else send(part_router, *hop) for hop in hops]

    scale_first = jnp.sqrt(total(squares(0, split, train, other)))
    own = [narrow(i, scale_first, 0, train, other) for i in range(FIRST)]
    own[0], own[1], train, other, *router_blocks = lax.optimization_barrier(
        (own[0], own[1], train, other, *router_blocks)
    )
    part_rest = squares(split, rows, train, other)
    part_rest, own[2] = lax.optimization_barrier((part_rest, own[2]))
    scale_rest = jnp.sqrt(total(part_rest))
    own += [narrow(i, scale_rest, split, train, other) for i in range(FIRST, len(PIECES))]

    high, _ = part_router.shape
    row_router = place(columns, router_blocks, None, 0, high, high)
    row_router, own[3] = lax.optimization_barrier((row_router, own[3]))
    all_router = lax.all_gather(row_router, "ep", axis=0, tiled=True)

    far, ready = {}, None
    for index in range(len(own) + 1):
        if index < len(own):
            if index >= 2:
                own[index], *far[index - 2] = lax.optimization_barrier((own[index], *far[index - 2]))
            if index >= 3:
                own[index], ready = lax.optimization_barrier((own[index], ready))
            if index == 5:
                own[index], all_router = lax.optimization_barrier((own[index], all_router))
                train, other, ready = lax.optimization_barrier((train, other, ready))
                latest_down = latest(0, rows, train, other)
            if index == 7:
                own[index], latest_down = lax.optimization_barrier((own[index], latest_down))
            far[index] = [send(own[index], hop, 0) for hop in range(1, chips)]
        done = index - 2
        for at in [done] if index < len(own) else [done, done + 1]:
            if at < 0:
                continue
            blocks = []
            for arrived in [own[at], *far[at]]:
                blocks += [arrived, send(arrived, 0, 1)]
            ready = place(columns, blocks, ready, edges[at], rows, step)

    latest_down = latest_down.reshape(experts, inner, width)
    serve_router = all_router.T

    scale_down = jnp.concatenate([scale_first, scale_rest]).reshape(experts, inner)
    return (ready.reshape(experts, inner, n * width), scale_down, serve_router, latest_down)


def solution(mesh):
    placed = (P("ep", None, "fsdp"), P("ep", None, "fsdp"), P("fsdp", "ep"), P("fsdp"))

    def body(*args):
        return on_device(mesh.shape["fsdp"], *args)

    return jax.shard_map(
        body,
        mesh=mesh,
        in_specs=placed,
        out_specs=(P("ep", None, None), P("ep", None), P(), P("ep", None, "fsdp")),
        check_vma=False,
    )
```
